32 devices in a mesh: rep: 16 (over z, y, core), tp: 2 (over x).
Axes of the slice: x: 2, y: 2, z: 4, core: 2. Of those that a mesh axis runs over, the one named last changes fastest.
Arguments:
- positions: int32 [4096], P('rep'), may hold values from 0 to 8191
- activations: bfloat16 [4096, 4096], P('rep', 'tp'), may hold values from -6 to 6
- norm_gain: bfloat16 [4096], P('tp'), may hold values from 0.5 to 1.5
- qkv_weight: bfloat16 [4096, 6144], P('rep', 'tp'), may hold values from -0.09375 to 0.09375
- gate_up_weight: bfloat16 [4096, 14336], P('rep', 'tp'), may hold values from -0.09375 to 0.09375
Outputs:
- qkv_out: bfloat16 [4096, 6144], P('rep', 'tp')
- hidden: bfloat16 [4096, 7168], P('rep', 'tp')
The draws below stay inside these ranges and needn't reach their ends.
All inputs are finite; a program needn't handle non-finite values.
Results may differ from the reference program's by a relative error of at most 0.0058.
Values may be sent and summed in bfloat16 or wider, within the bound.
A program may use at most 192 MiB of HBM per device.

```python
import jax
import jax.numpy as jnp
from jax import lax

D = 4096
QH = 32
KVH = 8
HD = 128
FF = 7168
QKV = 6144
TOTAL_SEQS = 4096
N_TP = 2


def with_ends(entries, rng, smallest, largest):
    shape = entries.shape
    index_at = [jax.random.randint(jax.random.fold_in(rng, axis), (), 0, shape[axis]) for axis in range(len(shape))]
    entries = entries.at[tuple(index_at)].set(smallest)
    longest = shape.index(max(shape))
    index_at[longest] = (index_at[longest] + 1) % shape[longest]
    return entries.at[tuple(index_at)].set(largest)


def steps_of(rng, extent, pieces, low, largest):
    def one(axis_at, shards_of):
        heights = jax.random.uniform(jax.random.fold_in(jax.random.fold_in(rng, 6), axis_at), (shards_of,), jnp.float32, low / len(pieces), largest / len(pieces))
        return jnp.repeat(jnp.exp(heights), extent[axis_at] // shards_of).reshape((-1,) + (1,) * (len(extent) - axis_at - 1))

    loudness = one(*pieces[0])
    for cut in pieces[1:]:
        loudness = loudness * one(*cut)
    return loudness


def gaussian(key, shape, scale, most, pieces=(), kind=jnp.bfloat16):
    entries = scale * jax.random.normal(key, shape, jnp.float32)
    if pieces:
        entries = entries * steps_of(key, shape, pieces, -0.22, 0.18)
    return jnp.clip(entries, -most, most).astype(kind)


def setup_inputs(seed: int = 0) -> dict:
    seeds = jax.random.split(jax.random.key(seed), 6)
    return {
        "positions": with_ends(jax.random.randint(seeds[0], (TOTAL_SEQS,), 0, 8192), jax.random.fold_in(seeds[0], 1), 0, 8191).astype(jnp.int32),
        "activations": gaussian(seeds[1], (TOTAL_SEQS, D), 1.0, 6.0, ((0, 16), (1, 2))),
        "norm_gain": jnp.clip(1.0 + 0.1 * jax.random.normal(seeds[2], (D,), jnp.float32), 0.5, 1.5).astype(jnp.bfloat16),
        "qkv_weight": gaussian(seeds[3], (D, QKV), D ** -0.5, 0.09375, ((0, 16), (1, 2))),
        "gate_up_weight": gaussian(seeds[4], (D, 2 * FF), D ** -0.5, 0.09375, ((0, 16), (1, 2))),
    }


theta_base = 500000.0
norm_eps = 1e-05

def normalize(gathered, gain_row):
    values = gathered.astype(jnp.float32)
    mean_square = lax.optimization_barrier(jnp.mean(values * values, axis=1, keepdims=True))
    return (values * lax.rsqrt(mean_square + norm_eps) * gain_row.astype(jnp.float32)).astype(jnp.bfloat16)

def rotary(joined_qkv, positions):
    row_count = joined_qkv.shape[0]
    per_group = QH // KVH + 2
    half_size = HD // 2
    head_view = joined_qkv.reshape(row_count, -1, per_group, HD)
    frequency = theta_base ** (-2.0 * jnp.arange(half_size, dtype=jnp.float32) / HD)
    angles = positions.astype(jnp.float32)[:, None] * frequency[None, :]
    cosine = jnp.cos(angles)[:, None, None, :]
    sine_part = jnp.sin(angles)[:, None, None, :]
    leading = head_view[..., :half_size]
    trailing = head_view[..., half_size:]
    turned = jnp.concatenate([leading * cosine - trailing * sine_part, trailing * cosine + leading * sine_part], axis=-1)
    rotated_mask = (jnp.arange(per_group) < per_group - 1)[None, None, :, None]
    return jnp.where(rotated_mask, turned, head_view).reshape(row_count, -1)

def reference(positions, activations, norm_gain, qkv_weight, gate_up_weight):
    normed = normalize(activations, norm_gain)
    joined_qkv = jnp.dot(normed, qkv_weight, preferred_element_type=jnp.float32)
    qkv_out = rotary(joined_qkv, positions).astype(jnp.bfloat16)
    gate_up = jnp.dot(normed, gate_up_weight, preferred_element_type=jnp.float32)
    row_count = gate_up.shape[0]
    paired = gate_up.reshape(row_count, N_TP, 2, FF // N_TP)
    hidden = (jax.nn.silu(paired[:, :, 0]) * paired[:, :, 1]).reshape(row_count, FF).astype(jnp.bfloat16)
    return (qkv_out, hidden)
```

```python
import functools

import jax
import jax.numpy as jnp
from jax import lax
from jax.experimental import pallas as pl
from jax.experimental.pallas import tpu as pltpu
from jax.sharding import PartitionSpec as P

QH = 32
KVH = 8
HD = 128
MESH = pl.DeviceIdType.MESH
CORES = 2
QUARTERS = 4

theta_base = 500000.0
norm_eps = 1e-05


def normalize(gathered, gain_row):
    values = gathered.astype(jnp.float32)
    mean_square = jnp.mean(values * values, axis=1, keepdims=True)
    return (values * lax.rsqrt(mean_square + norm_eps) * gain_row.astype(jnp.float32)).astype(
        jnp.bfloat16
    )


def angle_parts(positions):
    half_size = HD // 2
    frequency = theta_base ** (-2.0 * jnp.arange(half_size, dtype=jnp.float32) / HD)
    angles = positions.astype(jnp.float32)[:, None] * frequency[None, :]
    return jnp.cos(angles), jnp.sin(angles)


def rotary(joined_qkv, positions):
    row_count = joined_qkv.shape[0]
    per_group = QH // KVH + 2
    half_size = HD // 2
    head_view = joined_qkv.reshape(row_count, -1, per_group, HD)
    cosine, sine_part = angle_parts(positions)
    cosine = cosine[:, None, None, :]
    sine_part = sine_part[:, None, None, :]
    leading = head_view[..., :half_size]
    trailing = head_view[..., half_size:]
    turned = jnp.concatenate(
        [leading * cosine - trailing * sine_part, trailing * cosine + leading * sine_part], axis=-1
    )
    rotated_mask = (jnp.arange(per_group) < per_group - 1)[None, None, :, None]
    return jnp.where(rotated_mask, turned, head_view).reshape(row_count, -1)


def contract_rows(chosen, piece):
    return jnp.dot(chosen, piece, preferred_element_type=jnp.float32)


def plain(positions, activations, norm_gain, qkv_weight, gate_up_weight):
    features, gains = (
        lax.all_gather(activations, "tp", axis=1, tiled=True),
        lax.all_gather(norm_gain, "tp", axis=0, tiled=True),
    )
    normed = normalize(features, gains)
    seq_count = normed.shape[0]
    qkv_partial = contract_rows(normed, lax.all_gather(qkv_weight, "rep", axis=0, tiled=True))
    gateup_partial = contract_rows(
        normed, lax.all_gather(gate_up_weight, "rep", axis=0, tiled=True)
    )
    qkv_out = rotary(qkv_partial, positions).astype(jnp.bfloat16)
    paired = gateup_partial.reshape(seq_count, 2, -1)
    hidden = (jax.nn.silu(paired[:, 0]) * paired[:, 1]).astype(jnp.bfloat16)
    return (qkv_out, hidden)


def widths_of(total):
    widths = [256] * (total // 256)
    return widths + ([total % 256] if total % 256 else [])


def kernel(plan, table_in, x_in, gain_in, wq_in, wg_in, q_out, h_out, *scratch):
    (chips, seqs, feats, qcols, hcols, widths) = plan
    n_gu = len(widths)
    x_buf, t_buf, g_buf, q_res, wq_buf = scratch[:5]
    gu_bufs = scratch[5 : 5 + n_gu]
    h_res = scratch[5 + n_gu : 5 + 2 * n_gu]
    (w_send, w_recv, f_send, f_recv, o_send, o_recv, a_send, a_recv, l_sem) = scratch[5 + 2 * n_gu :]

    rep, t = lax.axis_index("rep"), lax.axis_index("tp")
    core = rep % CORES
    chip = rep // CORES
    half = chip // QUARTERS
    quarter = chip % QUARTERS
    zl, y = quarter // 2, quarter % 2

    def dev(other_chip, other_core=None, other_t=None):
        return (
            other_chip * CORES + (core if other_core is None else other_core),
            t if other_t is None else other_t,
        )

    sibling = dev(chip, 1 - core)
    across = dev(chip, core, 1 - t)
    z_peer = dev(half * QUARTERS + (1 - zl) * 2 + y)
    y_peer = dev(half * QUARTERS + zl * 2 + (1 - y))

    barrier = pltpu.get_barrier_semaphore()
    for k in range(1, chips):
        pl.semaphore_signal(barrier, inc=1, device_id=dev((chip + k) % chips), device_id_type=MESH)
    pl.semaphore_signal(barrier, inc=1, device_id=sibling, device_id_type=MESH)
    pl.semaphore_signal(barrier, inc=1, device_id=across, device_id_type=MESH)
    pl.semaphore_wait(barrier, chips + 1)

    def remote(src, dst, ssem, rsem, where):
        return pltpu.make_async_remote_copy(
            src_ref=src, dst_ref=dst, send_sem=ssem, recv_sem=rsem, device_id=where, device_id_type=MESH
        )

    def rows(index, count=1):
        return pl.ds(pl.multiple_of(index * seqs, seqs), count * seqs)

    def cols(base, width):
        return pl.ds(pl.multiple_of(base, HD), width)

    slot = y * 2 + zl
    mine = cols(t * feats, feats)
    theirs = cols((1 - t) * feats, feats)
    local = [
        pltpu.make_async_copy(x_in, x_buf.at[rows(slot), mine], l_sem.at[0]),
        pltpu.make_async_copy(table_in, t_buf.at[rows(slot)], l_sem.at[1]),
        pltpu.make_async_copy(gain_in, g_buf.at[:, mine], l_sem.at[2]),
    ]
    other = y * 2 + (1 - zl)
    z_x = remote(x_in, x_buf.at[rows(slot), mine], a_send.at[0], a_recv.at[0], z_peer)
    z_t = remote(table_in, t_buf.at[rows(slot)], a_send.at[1], a_recv.at[1], z_peer)
    x_own = remote(x_in, x_buf.at[rows(slot), mine], a_send.at[2], a_recv.at[2], across)
    x_gain = remote(gain_in, g_buf.at[:, mine], a_send.at[3], a_recv.at[3], across)
    y_own = remote(x_in, x_buf.at[rows(slot), mine], a_send.at[4], a_recv.at[4], y_peer)
    y_t = remote(table_in, t_buf.at[rows(slot)], a_send.at[5], a_recv.at[5], y_peer)
    y_two = remote(x_buf.at[rows(other), mine], x_buf.at[rows(other), mine], a_send.at[6], a_recv.at[6], y_peer)
    y_t2 = remote(t_buf.at[rows(other)], t_buf.at[rows(other)], a_send.at[7], a_recv.at[7], y_peer)
    x_two = remote(x_buf.at[rows(other), mine], x_buf.at[rows(other), mine], a_send.at[8], a_recv.at[8], across)
    far = (1 - y) * 2 + zl
    far2 = (1 - y) * 2 + (1 - zl)
    x_three = remote(x_buf.at[rows(far), mine], x_buf.at[rows(far), mine], a_send.at[9], a_recv.at[9], across)
    x_four = remote(x_buf.at[rows(far2), mine], x_buf.at[rows(far2), mine], a_send.at[10], a_recv.at[10], across)

    pieces = [(wq_in, lambda q: q * qcols, qcols, wq_buf, 0)]
    chunks = [[0]]
    at = 0
    for n, width in enumerate(widths):
        for part in range(2):
            base = part * hcols * QUARTERS + at
            pieces.append((wg_in, lambda q, base=base: base + q * hcols, width, gu_bufs[n], part * width))
        chunks.append([2 * n + 1, 2 * n + 2])
        at += width

    def piece_src(p, q):
        src, col, width, _, _ = pieces[p]
        return src.at[:, cols(col(q), width)]

    def piece_dst(p, owner_rep):
        _, _, width, buf, col = pieces[p]
        return buf.at[rows(owner_rep), col : col + width]

    order = [(k + chips // 2) % chips for k in range(chips)]
    order = [k for k in order if k]

    def weight_send(p, k):
        to = (chip + k) % chips
        return remote(
            piece_src(p, to % QUARTERS), piece_dst(p, rep), w_send.at[p, k], w_recv.at[p, chip], dev(to)
        )

    def weight_from(p, k):
        source = (chip + chips - k) % chips
        owner = source * CORES + core
        return remote(
            piece_dst(p, owner), piece_dst(p, owner), w_send.at[p, k], w_recv.at[p, source], dev(source)
        )

    def own_local(p):
        return pltpu.make_async_copy(piece_src(p, quarter), piece_dst(p, rep), l_sem.at[3 + p])

    def own_pass(p):
        return remote(piece_src(p, quarter), piece_dst(p, rep), f_send.at[p, 0], f_recv.at[p, 0], sibling)

    def passed(p, k):
        source = (chip + chips - k) % chips
        owner = source * CORES + core
        return remote(piece_dst(p, owner), piece_dst(p, owner), f_send.at[p, k], f_recv.at[p, k], sibling)

    def passed_in(p, k):
        source = (chip + chips - k) % chips
        owner = source * CORES + (1 - core)
        return remote(piece_dst(p, owner), piece_dst(p, owner), f_send.at[p, k], f_recv.at[p, k], sibling)

    def start_chunk(c):
        for k in order:
            for p in chunks[c]:
                weight_send(p, k).start()
        for p in chunks[c]:
            own_local(p).start()
            own_pass(p).start()

    def pass_chunk(c):
        for k in order:
            for p in chunks[c]:
                weight_from(p, k).wait_recv()
                passed(p, k).start()

    def finish_chunk(c):
        for p in chunks[c]:
            own_local(p).wait()
            for k in range(chips):
                passed_in(p, k).wait_recv()

    for copy in (z_x, z_t, x_own, x_gain, y_own, y_t, *local):
        copy.start()
    start_chunk(0)
    z_x.wait_recv()
    y_two.start()
    x_two.start()
    z_t.wait_recv()
    y_t2.start()
    for c in range(1, len(chunks)):
        start_chunk(c)
    y_own.wait_recv()
    x_three.start()
    y_two.wait_recv()
    x_four.start()
    pass_chunk(0)
    for copy in (y_t, y_t2, x_own, x_gain, x_two, x_three, x_four):
        copy.wait_recv()
    for copy in local:
        copy.wait()
    for copy in (z_x, z_t, x_own, x_gain, y_own, y_t, y_two, y_t2, x_two, x_three, x_four):
        copy.wait_send()

    total = QUARTERS * seqs
    tall = 32

    @pl.loop(0, total // tall)
    def _(i):
        at_rows = pl.ds(pl.multiple_of(i * tall, tall), tall)
        values = x_buf[at_rows, :].astype(jnp.float32)
        mean_square = jnp.mean(values * values, axis=1, keepdims=True)
        x_buf[at_rows, :] = (values * lax.rsqrt(mean_square + norm_eps) * g_buf[...]).astype(jnp.bfloat16)

    per_group = QH // KVH + 2
    deep = 2 * seqs

    def compute(c):
        @pl.loop(0, total // deep)
        def _(i):
            at_rows = pl.ds(pl.multiple_of(i * deep, deep), deep)
            chosen = x_buf[at_rows, :]
            if c == 0:
                table = t_buf[at_rows, :]
                swapped = pltpu.roll(table, HD // 2, 1)
                lane = lax.broadcasted_iota(jnp.int32, table.shape, 1)
                low = lane < HD // 2
                cosine = jnp.where(low, table, swapped)
                sine_part = jnp.where(low, -swapped, table)
                for n in range(0, qcols, 2 * HD):
                    wide = jnp.dot(chosen, wq_buf[:, n : n + 2 * HD], preferred_element_type=jnp.float32)
                    for s in range(2):
                        head = wide[:, s * HD : (s + 1) * HD]
                        if (n // HD + s) % per_group < per_group - 1:
                            head = head * cosine + pltpu.roll(head, HD // 2, 1) * sine_part
                        q_res[at_rows, n + s * HD : n + (s + 1) * HD] = head.astype(jnp.bfloat16)
            else:
                width = widths[c - 1]
                both = jnp.dot(chosen, gu_bufs[c - 1][...], preferred_element_type=jnp.float32)
                gate, up = both[:, :width], both[:, width:]
                h_res[c - 1][at_rows, :] = (gate / (1.0 + jnp.exp(-gate)) * up).astype(jnp.bfloat16)

    def result(c, q):
        place = (q % 2) * 2 + q // 2
        if c == 0:
            return q_res.at[rows(place)], lambda mover: q_out.at[:, cols(mover * qcols, qcols)]
        offset = sum(widths[: c - 1])
        return h_res[c - 1].at[rows(place)], lambda mover: h_out.at[:, cols(mover * hcols + offset, widths[c - 1])]

    def out_send(c, k):
        to = (quarter + k) % QUARTERS
        src, dst = result(c, to)
        return remote(src, dst(quarter), o_send.at[c, k], o_recv.at[c, k], dev(half * QUARTERS + to))

    def out_from(c, k):
        source = (quarter + QUARTERS - k) % QUARTERS
        src, dst = result(c, quarter)
        return remote(src, dst(source), o_send.at[c, k], o_recv.at[c, k], dev(half * QUARTERS + source))

    def out_local(c):
        src, dst = result(c, quarter)
        return pltpu.make_async_copy(src, dst(quarter), l_sem.at[3 + len(pieces) + c])

    def ship(c):
        for k in range(1, QUARTERS):
            out_send(c, k).start()
        out_local(c).start()

    for c in range(len(chunks)):
        if c + 1 < len(chunks):
            pass_chunk(c + 1)
        finish_chunk(c)
        compute(c)
        ship(c)

    for c in range(len(chunks)):
        for p in chunks[c]:
            for k in range(1, chips):
                weight_send(p, k).wait_send()
                passed(p, k).wait_send()
            own_pass(p).wait_send()
        out_local(c).wait()
        for k in range(1, QUARTERS):
            out_send(c, k).wait_send()
            out_from(c, k).wait_recv()


def fused(chips, positions, activations, norm_gain, qkv_weight, gate_up_weight):
    seqs, feats = activations.shape
    depth, qkv_cols = qkv_weight.shape
    qcols = qkv_cols // QUARTERS
    hcols = gate_up_weight.shape[1] // 2 // QUARTERS
    widths = widths_of(hcols)
    rank = chips * CORES
    table = jnp.concatenate(angle_parts(positions), axis=1)
    gains = norm_gain.astype(jnp.float32)[None, :]
    bf16, f32 = jnp.bfloat16, jnp.float32
    pieces, chunks = 1 + 2 * len(widths), 1 + len(widths)
    dma = pltpu.SemaphoreType.DMA
    scratch = [
        pltpu.VMEM((QUARTERS * seqs, 2 * feats), bf16),
        pltpu.VMEM((QUARTERS * seqs, HD), f32),
        pltpu.VMEM((1, 2 * feats), f32),
        pltpu.VMEM((QUARTERS * seqs, qcols), bf16),
        pltpu.VMEM((rank * depth, qcols), bf16),
        *[pltpu.VMEM((rank * depth, 2 * w), bf16) for w in widths],
        *[pltpu.VMEM((QUARTERS * seqs, w), bf16) for w in widths],
        dma((pieces, chips)),
        dma((pieces, chips)),
        dma((pieces, chips)),
        dma((pieces, chips)),
        dma((chunks, QUARTERS)),
        dma((chunks, QUARTERS)),
        dma((11,)),
        dma((11,)),
        dma((3 + pieces + chunks,)),
    ]
    plan = (chips, seqs, feats, qcols, hcols, tuple(widths))
    anywhere = pl.BlockSpec(memory_space=pl.ANY)
    return pl.pallas_call(
        functools.partial(kernel, plan),
        out_shape=(
            jax.ShapeDtypeStruct((seqs, qkv_cols), bf16),
            jax.ShapeDtypeStruct((seqs, hcols * QUARTERS), bf16),
        ),
        in_specs=[anywhere] * 5,
        out_specs=(anywhere, anywhere),
        scratch_shapes=scratch,
        compiler_params=pltpu.CompilerParams(
            collective_id=0, has_side_effects=True, vmem_limit_bytes=60 * 1024 * 1024
        ),
    )(table, activations, gains, qkv_weight, gate_up_weight)


def per_device(reps, tps, positions, activations, norm_gain, qkv_weight, gate_up_weight):
    chips = reps // CORES
    seqs, depth = activations.shape[0], qkv_weight.shape[0]
    fits = (
        chips == 2 * QUARTERS
        and tps == 2
        and seqs == depth
        and seqs % 32 == 0
        and qkv_weight.shape[1] % (QUARTERS * (QH // KVH + 2) * HD) == 0
        and gate_up_weight.shape[1] % (2 * QUARTERS * HD) == 0
    )
    step = functools.partial(fused, chips) if fits else plain
    return step(positions, activations, norm_gain, qkv_weight, gate_up_weight)


def solution(mesh):
    placed = (P("rep"), P("rep", "tp"), P("tp"), P("rep", "tp"), P("rep", "tp"))
    return jax.shard_map(
        functools.partial(per_device, mesh.shape["rep"], mesh.shape["tp"]),
        mesh=mesh,
        in_specs=placed,
        out_specs=(P("rep", "tp"), P("rep", "tp")),
        check_vma=False,
    )
```

```python
import functools

import jax
import jax.numpy as jnp
from jax import lax
from jax.experimental import pallas as pl
from jax.experimental.pallas import tpu as pltpu
from jax.sharding import PartitionSpec as P

QH = 32
KVH = 8
HD = 128
MESH = pl.DeviceIdType.MESH
CORES = 2
QUARTERS = 4

theta_base = 500000.0
norm_eps = 1e-05


def normalize(gathered, gain_row):
    values = gathered.astype(jnp.float32)
    mean_square = jnp.mean(values * values, axis=1, keepdims=True)
    return (values * lax.rsqrt(mean_square + norm_eps) * gain_row.astype(jnp.float32)).astype(
        jnp.bfloat16
    )


def angle_parts(positions):
    half_size = HD // 2
    frequency = theta_base ** (-2.0 * jnp.arange(half_size, dtype=jnp.float32) / HD)
    angles = positions.astype(jnp.float32)[:, None] * frequency[None, :]
    return jnp.cos(angles), jnp.sin(angles)


def rotary(joined_qkv, positions):
    row_count = joined_qkv.shape[0]
    per_group = QH // KVH + 2
    half_size = HD // 2
    head_view = joined_qkv.reshape(row_count, -1, per_group, HD)
    cosine, sine_part = angle_parts(positions)
    cosine = cosine[:, None, None, :]
    sine_part = sine_part[:, None, None, :]
    leading = head_view[..., :half_size]
    trailing = head_view[..., half_size:]
    turned = jnp.concatenate(
        [leading * cosine - trailing * sine_part, trailing * cosine + leading * sine_part], axis=-1
    )
    rotated_mask = (jnp.arange(per_group) < per_group - 1)[None, None, :, None]
    return jnp.where(rotated_mask, turned, head_view).reshape(row_count, -1)


def contract_rows(chosen, piece):
    return jnp.dot(chosen, piece, preferred_element_type=jnp.float32)


def plain(positions, activations, norm_gain, qkv_weight, gate_up_weight):
    features, gains = (
        lax.all_gather(activations, "tp", axis=1, tiled=True),
        lax.all_gather(norm_gain, "tp", axis=0, tiled=True),
    )
    normed = normalize(features, gains)
    seq_count = normed.shape[0]
    qkv_partial = contract_rows(normed, lax.all_gather(qkv_weight, "rep", axis=0, tiled=True))
    gateup_partial = contract_rows(
        normed, lax.all_gather(gate_up_weight, "rep", axis=0, tiled=True)
    )
    qkv_out = rotary(qkv_partial, positions).astype(jnp.bfloat16)
    paired = gateup_partial.reshape(seq_count, 2, -1)
    hidden = (jax.nn.silu(paired[:, 0]) * paired[:, 1]).astype(jnp.bfloat16)
    return (qkv_out, hidden)


def widths_of(total):
    widths = [256] * (total // 256)
    return widths + ([total % 256] if total % 256 else [])


def kernel(plan, table_in, x_in, gain_in, wq_in, wg_in, q_out, h_out, *scratch):
    (chips, seqs, feats, qcols, hcols, widths) = plan
    n_gu = len(widths)
    x_buf, t_buf, g_buf, q_res, wq_buf = scratch[:5]
    gu_bufs = scratch[5 : 5 + n_gu]
    h_res = scratch[5 + n_gu : 5 + 2 * n_gu]
    (w_send, w_recv, f_send, f_recv, o_send, o_recv, a_send, a_recv, l_sem) = scratch[5 + 2 * n_gu :]

    rep, t = lax.axis_index("rep"), lax.axis_index("tp")
    core = rep % CORES
    chip = rep // CORES
    half = chip // QUARTERS
    quarter = chip % QUARTERS
    zl, y = quarter // 2, quarter % 2

    def dev(other_chip, other_core=None, other_t=None):
        return (
            other_chip * CORES + (core if other_core is None else other_core),
            t if other_t is None else other_t,
        )

    sibling = dev(chip, 1 - core)
    across = dev(chip, core, 1 - t)
    z_peer = dev(half * QUARTERS + (1 - zl) * 2 + y)
    y_peer = dev(half * QUARTERS + zl * 2 + (1 - y))

    barrier = pltpu.get_barrier_semaphore()
    for k in range(1, chips):
        pl.semaphore_signal(barrier, inc=1, device_id=dev((chip + k) % chips), device_id_type=MESH)
    pl.semaphore_signal(barrier, inc=1, device_id=sibling, device_id_type=MESH)
    pl.semaphore_signal(barrier, inc=1, device_id=across, device_id_type=MESH)
    pl.semaphore_wait(barrier, chips + 1)

    def remote(src, dst, ssem, rsem, where):
        return pltpu.make_async_remote_copy(
            src_ref=src, dst_ref=dst, send_sem=ssem, recv_sem=rsem, device_id=where, device_id_type=MESH
        )

    def rows(index, count=1):
        return pl.ds(pl.multiple_of(index * seqs, seqs), count * seqs)

    def cols(base, width):
        return pl.ds(pl.multiple_of(base, HD), width)

    slot = y * 2 + zl
    mine = cols(t * feats, feats)
    theirs = cols((1 - t) * feats, feats)
    local = [
        pltpu.make_async_copy(x_in, x_buf.at[rows(slot), mine], l_sem.at[0]),
        pltpu.make_async_copy(table_in, t_buf.at[rows(slot)], l_sem.at[1]),
        pltpu.make_async_copy(gain_in, g_buf.at[mine], l_sem.at[2]),
    ]
    other = y * 2 + (1 - zl)
    z_x = remote(x_in, x_buf.at[rows(slot), mine], a_send.at[0], a_recv.at[0], z_peer)
    z_t = remote(table_in, t_buf.at[rows(slot)], a_send.at[1], a_recv.at[1], z_peer)
    x_own = remote(x_in, x_buf.at[rows(slot), mine], a_send.at[2], a_recv.at[2], across)
    x_gain = remote(gain_in, g_buf.at[mine], a_send.at[3], a_recv.at[3], across)
    y_own = remote(x_in, x_buf.at[rows(slot), mine], a_send.at[4], a_recv.at[4], y_peer)
    y_t = remote(table_in, t_buf.at[rows(slot)], a_send.at[5], a_recv.at[5], y_peer)
    y_two = remote(x_buf.at[rows(other), mine], x_buf.at[rows(other), mine], a_send.at[6], a_recv.at[6], y_peer)
    y_t2 = remote(t_buf.at[rows(other)], t_buf.at[rows(other)], a_send.at[7], a_recv.at[7], y_peer)
    x_two = remote(x_buf.at[rows(other), mine], x_buf.at[rows(other), mine], a_send.at[8], a_recv.at[8], across)
    far = (1 - y) * 2 + zl
    far2 = (1 - y) * 2 + (1 - zl)
    x_three = remote(x_buf.at[rows(far), mine], x_buf.at[rows(far), mine], a_send.at[9], a_recv.at[9], across)
    x_four = remote(x_buf.at[rows(far2), mine], x_buf.at[rows(far2), mine], a_send.at[10], a_recv.at[10], across)

    pieces = [(wq_in, lambda q: q * qcols, qcols, wq_buf, 0)]
    chunks = [[0]]
    at = 0
    for n, width in enumerate(widths):
        for part in range(2):
            base = part * hcols * QUARTERS + at
            pieces.append((wg_in, lambda q, base=base: base + q * hcols, width, gu_bufs[n], part * width))
        chunks.append([2 * n + 1, 2 * n + 2])
        at += width

    def piece_src(p, q):
        src, col, width, _, _ = pieces[p]
        return src.at[:, cols(col(q), width)]

    def piece_dst(p, owner_rep):
        _, _, width, buf, col = pieces[p]
        return buf.at[rows(owner_rep), col : col + width]

    order = [(k + chips // 2) % chips for k in range(chips)]
    order = [k for k in order if k]

    def weight_send(p, k):
        to = (chip + k) % chips
        return remote(
            piece_src(p, to % QUARTERS), piece_dst(p, rep), w_send.at[p, k], w_recv.at[p, chip], dev(to)
        )

    def weight_from(p, k):
        source = (chip + chips - k) % chips
        owner = source * CORES + core
        return remote(
            piece_dst(p, owner), piece_dst(p, owner), w_send.at[p, k], w_recv.at[p, source], dev(source)
        )

    def own_local(p):
        return pltpu.make_async_copy(piece_src(p, quarter), piece_dst(p, rep), l_sem.at[3 + p])

    def own_pass(p):
        return remote(piece_src(p, quarter), piece_dst(p, rep), f_send.at[p, 0], f_recv.at[p, 0], sibling)

    def passed(p, k):
        source = (chip + chips - k) % chips
        owner = source * CORES + core
        return remote(piece_dst(p, owner), piece_dst(p, owner), f_send.at[p, k], f_recv.at[p, k], sibling)

    def passed_in(p, k):
        source = (chip + chips - k) % chips
        owner = source * CORES + (1 - core)
        return remote(piece_dst(p, owner), piece_dst(p, owner), f_send.at[p, k], f_recv.at[p, k], sibling)

    def start_chunk(c):
        for k in order:
            for p in chunks[c]:
                weight_send(p, k).start()
        for p in chunks[c]:
            own_local(p).start()
            own_pass(p).start()

    def pass_chunk(c):
        for k in order:
            for p in chunks[c]:
                weight_from(p, k).wait_recv()
                passed(p, k).start()

    def finish_chunk(c):
        for p in chunks[c]:
            own_local(p).wait()
            for k in range(chips):
                passed_in(p, k).wait_recv()

    for copy in (z_x, z_t, x_own, x_gain, y_own, y_t, *local):
        copy.start()
    start_chunk(0)
    z_x.wait_recv()
    y_two.start()
    x_two.start()
    z_t.wait_recv()
    y_t2.start()
    for c in range(1, len(chunks)):
        start_chunk(c)
    y_own.wait_recv()
    x_three.start()
    y_two.wait_recv()
    x_four.start()
    pass_chunk(0)
    for copy in (y_t, y_t2, x_own, x_gain, x_two, x_three, x_four):
        copy.wait_recv()
    for copy in local:
        copy.wait()
    for copy in (z_x, z_t, x_own, x_gain, y_own, y_t, y_two, y_t2, x_two, x_three, x_four):
        copy.wait_send()

    total = QUARTERS * seqs
    tall = 32

    gain_row = g_buf[...].astype(jnp.float32)[None, :]

    @pl.loop(0, total // tall)
    def _(i):
        at_rows = pl.ds(pl.multiple_of(i * tall, tall), tall)
        values = x_buf[at_rows, :].astype(jnp.float32)
        mean_square = jnp.mean(values * values, axis=1, keepdims=True)
        x_buf[at_rows, :] = (values * lax.rsqrt(mean_square + norm_eps) * gain_row).astype(jnp.bfloat16)

    per_group = QH // KVH + 2
    deep = 2 * seqs

    def compute(c):
        @pl.loop(0, total // deep)
        def _(i):
            at_rows = pl.ds(pl.multiple_of(i * deep, deep), deep)
            chosen = x_buf[at_rows, :]
            if c == 0:
                table = t_buf[at_rows, :]
                swapped = pltpu.roll(table, HD // 2, 1)
                lane = lax.broadcasted_iota(jnp.int32, table.shape, 1)
                low = lane < HD // 2
                cosine = jnp.where(low, table, swapped)
                sine_part = jnp.where(low, -swapped, table)
                for n in range(0, qcols, 2 * HD):
                    wide = jnp.dot(chosen, wq_buf[:, n : n + 2 * HD], preferred_element_type=jnp.float32)
                    for s in range(2):
                        head = wide[:, s * HD : (s + 1) * HD]
                        if (n // HD + s) % per_group < per_group - 1:
                            head = head * cosine + pltpu.roll(head, HD // 2, 1) * sine_part
                        q_res[at_rows, n + s * HD : n + (s + 1) * HD] = head.astype(jnp.bfloat16)
            else:
                width = widths[c - 1]
                both = jnp.dot(chosen, gu_bufs[c - 1][...], preferred_element_type=jnp.float32)
                gate, up = both[:, :width], both[:, width:]
                h_res[c - 1][at_rows, :] = (gate / (1.0 + jnp.exp(-gate)) * up).astype(jnp.bfloat16)

    def result(c, q):
        place = (q % 2) * 2 + q // 2
        if c == 0:
            return q_res.at[rows(place)], lambda mover: q_out.at[:, cols(mover * qcols, qcols)]
        offset = sum(widths[: c - 1])
        return h_res[c - 1].at[rows(place)], lambda mover: h_out.at[:, cols(mover * hcols + offset, widths[c - 1])]

    def out_send(c, k):
        to = (quarter + k) % QUARTERS
        src, dst = result(c, to)
        return remote(src, dst(quarter), o_send.at[c, k], o_recv.at[c, k], dev(half * QUARTERS + to))

    def out_from(c, k):
        source = (quarter + QUARTERS - k) % QUARTERS
        src, dst = result(c, quarter)
        return remote(src, dst(source), o_send.at[c, k], o_recv.at[c, k], dev(half * QUARTERS + source))

    def out_local(c):
        src, dst = result(c, quarter)
        return pltpu.make_async_copy(src, dst(quarter), l_sem.at[3 + len(pieces) + c])

    def ship(c):
        for k in range(1, QUARTERS):
            out_send(c, k).start()
        out_local(c).start()

    for c in range(len(chunks)):
        if c:
            pass_chunk(c)
        finish_chunk(c)
        compute(c)
        ship(c)
        if c + 99 < len(chunks):
            start_chunk(c + 99)

    for c in range(len(chunks)):
        for p in chunks[c]:
            for k in range(1, chips):
                weight_send(p, k).wait_send()
                passed(p, k).wait_send()
            own_pass(p).wait_send()
        out_local(c).wait()
        for k in range(1, QUARTERS):
            out_send(c, k).wait_send()
            out_from(c, k).wait_recv()


def fused(chips, positions, activations, norm_gain, qkv_weight, gate_up_weight):
    seqs, feats = activations.shape
    depth, qkv_cols = qkv_weight.shape
    qcols = qkv_cols // QUARTERS
    hcols = gate_up_weight.shape[1] // 2 // QUARTERS
    widths = widths_of(hcols)
    rank = chips * CORES
    table = jnp.concatenate(angle_parts(positions), axis=1)
    gains = norm_gain
    bf16, f32 = jnp.bfloat16, jnp.float32
    pieces, chunks = 1 + 2 * len(widths), 1 + len(widths)
    dma = pltpu.SemaphoreType.DMA
    scratch = [
        pltpu.VMEM((QUARTERS * seqs, 2 * feats), bf16),
        pltpu.VMEM((QUARTERS * seqs, HD), f32),
        pltpu.VMEM((2 * feats,), bf16),
        pltpu.VMEM((QUARTERS * seqs, qcols), bf16),
        pltpu.VMEM((rank * depth, qcols), bf16),
        *[pltpu.VMEM((rank * depth, 2 * w), bf16) for w in widths],
        *[pltpu.VMEM((QUARTERS * seqs, w), bf16) for w in widths],
        dma((pieces, chips)),
        dma((pieces, chips)),
        dma((pieces, chips)),
        dma((pieces, chips)),
        dma((chunks, QUARTERS)),
        dma((chunks, QUARTERS)),
        dma((11,)),
        dma((11,)),
        dma((3 + pieces + chunks,)),
    ]
    plan = (chips, seqs, feats, qcols, hcols, tuple(widths))
    anywhere = pl.BlockSpec(memory_space=pl.ANY)
    return pl.pallas_call(
        functools.partial(kernel, plan),
        out_shape=(
            pltpu.VMEM((seqs, qkv_cols), bf16),
            pltpu.VMEM((seqs, hcols * QUARTERS), bf16),
        ),
        in_specs=[anywhere] * 5,
        out_specs=(pl.BlockSpec(memory_space=pltpu.VMEM), pl.BlockSpec(memory_space=pltpu.VMEM)),
        scratch_shapes=scratch,
        compiler_params=pltpu.CompilerParams(
            collective_id=0, has_side_effects=True, vmem_limit_bytes=60 * 1024 * 1024
        ),
    )(table, activations, gains, qkv_weight, gate_up_weight)


def per_device(reps, tps, positions, activations, norm_gain, qkv_weight, gate_up_weight):
    chips = reps // CORES
    seqs, depth = activations.shape[0], qkv_weight.shape[0]
    fits = (
        chips == 2 * QUARTERS
        and tps == 2
        and seqs == depth
        and seqs % 32 == 0
        and qkv_weight.shape[1] % (QUARTERS * (QH // KVH + 2) * HD) == 0
        and gate_up_weight.shape[1] % (2 * QUARTERS * HD) == 0
    )
    step = functools.partial(fused, chips) if fits else plain
    return step(positions, activations, norm_gain, qkv_weight, gate_up_weight)


def solution(mesh):
    placed = (P("rep"), P("rep", "tp"), P("tp"), P("rep", "tp"), P("rep", "tp"))
    return jax.shard_map(
        functools.partial(per_device, mesh.shape["rep"], mesh.shape["tp"]),
        mesh=mesh,
        in_specs=placed,
        out_specs=(P("rep", "tp"), P("rep", "tp")),
        check_vma=False,
    )
```

```python
import functools

import jax
import jax.numpy as jnp
from jax import lax
from jax.experimental import pallas as pl
from jax.experimental.pallas import tpu as pltpu
from jax.sharding import PartitionSpec as P

QH = 32
KVH = 8
HD = 128
MESH = pl.DeviceIdType.MESH
CORES = 2
QUARTERS = 4

theta_base = 500000.0
norm_eps = 1e-05


def normalize(gathered, gain_row):
    values = gathered.astype(jnp.float32)
    mean_square = jnp.mean(values * values, axis=1, keepdims=True)
    return (values * lax.rsqrt(mean_square + norm_eps) * gain_row.astype(jnp.float32)).astype(
        jnp.bfloat16
    )


def angle_parts(positions):
    half_size = HD // 2
    frequency = theta_base ** (-2.0 * jnp.arange(half_size, dtype=jnp.float32) / HD)
    angles = positions.astype(jnp.float32)[:, None] * frequency[None, :]
    return jnp.cos(angles), jnp.sin(angles)


def rotary(joined_qkv, positions):
    row_count = joined_qkv.shape[0]
    per_group = QH // KVH + 2
    half_size = HD // 2
    head_view = joined_qkv.reshape(row_count, -1, per_group, HD)
    cosine, sine_part = angle_parts(positions)
    cosine = cosine[:, None, None, :]
    sine_part = sine_part[:, None, None, :]
    leading = head_view[..., :half_size]
    trailing = head_view[..., half_size:]
    turned = jnp.concatenate(
        [leading * cosine - trailing * sine_part, trailing * cosine + leading * sine_part], axis=-1
    )
    rotated_mask = (jnp.arange(per_group) < per_group - 1)[None, None, :, None]
    return jnp.where(rotated_mask, turned, head_view).reshape(row_count, -1)


def contract_rows(chosen, piece):
    return jnp.dot(chosen, piece, preferred_element_type=jnp.float32)


def plain(positions, activations, norm_gain, qkv_weight, gate_up_weight):
    features, gains = (
        lax.all_gather(activations, "tp", axis=1, tiled=True),
        lax.all_gather(norm_gain, "tp", axis=0, tiled=True),
    )
    normed = normalize(features, gains)
    seq_count = normed.shape[0]
    qkv_partial = contract_rows(normed, lax.all_gather(qkv_weight, "rep", axis=0, tiled=True))
    gateup_partial = contract_rows(
        normed, lax.all_gather(gate_up_weight, "rep", axis=0, tiled=True)
    )
    qkv_out = rotary(qkv_partial, positions).astype(jnp.bfloat16)
    paired = gateup_partial.reshape(seq_count, 2, -1)
    hidden = (jax.nn.silu(paired[:, 0]) * paired[:, 1]).astype(jnp.bfloat16)
    return (qkv_out, hidden)


def widths_of(total):
    blocks = total // HD
    tail = min(3, blocks)
    wide, left = divmod(blocks - tail, QUARTERS)
    return [QUARTERS * HD] * wide + ([left * HD] if left else []) + [HD] * tail


def kernel(plan, table_in, x_in, gain_in, wq_in, wg_in, q_out, h_out, *scratch):
    (chips, seqs, feats, qcols, hcols, widths) = plan
    n_gu = len(widths)
    x_buf, t_buf, g_buf, q_res, wq_buf = scratch[:5]
    gu_bufs = scratch[5 : 5 + n_gu]
    h_res = scratch[5 + n_gu : 5 + 2 * n_gu]
    (w_send, w_recv, f_send, f_recv, o_send, o_recv, a_send, a_recv, l_sem) = scratch[5 + 2 * n_gu :]

    rep, t = lax.axis_index("rep"), lax.axis_index("tp")
    core = rep % CORES
    chip = rep // CORES
    half = chip // QUARTERS
    quarter = chip % QUARTERS
    zl, y = quarter // 2, quarter % 2

    def dev(other_chip, other_core=None, other_t=None):
        return (
            other_chip * CORES + (core if other_core is None else other_core),
            t if other_t is None else other_t,
        )

    sibling = dev(chip, 1 - core)
    across = dev(chip, core, 1 - t)
    z_peer = dev(half * QUARTERS + (1 - zl) * 2 + y)
    y_peer = dev(half * QUARTERS + zl * 2 + (1 - y))

    barrier = pltpu.get_barrier_semaphore()
    for k in range(1, chips):
        pl.semaphore_signal(barrier, inc=1, device_id=dev((chip + k) % chips), device_id_type=MESH)
    pl.semaphore_signal(barrier, inc=1, device_id=sibling, device_id_type=MESH)
    pl.semaphore_signal(barrier, inc=1, device_id=across, device_id_type=MESH)
    pl.semaphore_wait(barrier, chips + 1)

    def remote(src, dst, ssem, rsem, where):
        return pltpu.make_async_remote_copy(
            src_ref=src, dst_ref=dst, send_sem=ssem, recv_sem=rsem, device_id=where, device_id_type=MESH
        )

    def rows(index, count=1):
        return pl.ds(pl.multiple_of(index * seqs, seqs), count * seqs)

    def cols(base, width):
        return pl.ds(pl.multiple_of(base, HD), width)

    slot = y * 2 + zl
    mine = cols(t * feats, feats)
    theirs = cols((1 - t) * feats, feats)
    local = [
        pltpu.make_async_copy(x_in, x_buf.at[rows(slot), mine], l_sem.at[0]),
        pltpu.make_async_copy(table_in, t_buf.at[rows(slot)], l_sem.at[1]),
        pltpu.make_async_copy(gain_in, g_buf.at[mine], l_sem.at[2]),
    ]
    other = y * 2 + (1 - zl)
    z_x = remote(x_in, x_buf.at[rows(slot), mine], a_send.at[0], a_recv.at[0], z_peer)
    z_t = remote(table_in, t_buf.at[rows(slot)], a_send.at[1], a_recv.at[1], z_peer)
    x_own = remote(x_in, x_buf.at[rows(slot), mine], a_send.at[2], a_recv.at[2], across)
    x_gain = remote(gain_in, g_buf.at[mine], a_send.at[3], a_recv.at[3], across)
    y_own = remote(x_in, x_buf.at[rows(slot), mine], a_send.at[4], a_recv.at[4], y_peer)
    y_t = remote(table_in, t_buf.at[rows(slot)], a_send.at[5], a_recv.at[5], y_peer)
    y_two = remote(x_buf.at[rows(other), mine], x_buf.at[rows(other), mine], a_send.at[6], a_recv.at[6], y_peer)
    y_t2 = remote(t_buf.at[rows(other)], t_buf.at[rows(other)], a_send.at[7], a_recv.at[7], y_peer)
    x_two = remote(x_buf.at[rows(other), mine], x_buf.at[rows(other), mine], a_send.at[8], a_recv.at[8], across)
    far = (1 - y) * 2 + zl
    far2 = (1 - y) * 2 + (1 - zl)
    x_three = remote(x_buf.at[rows(far), mine], x_buf.at[rows(far), mine], a_send.at[9], a_recv.at[9], across)
    x_four = remote(x_buf.at[rows(far2), mine], x_buf.at[rows(far2), mine], a_send.at[10], a_recv.at[10], across)

    pieces = [(wq_in, lambda q: q * qcols, qcols, wq_buf, 0)]
    chunks = [[0]]
    at = 0
    for n, width in enumerate(widths):
        for part in range(2):
            base = part * hcols * QUARTERS + at
            pieces.append((wg_in, lambda q, base=base: base + q * hcols, width, gu_bufs[n], part * width))
        chunks.append([2 * n + 1, 2 * n + 2])
        at += width

    def piece_src(p, q):
        src, col, width, _, _ = pieces[p]
        return src.at[:, cols(col(q), width)]

    def piece_dst(p, owner_rep):
        _, _, width, buf, col = pieces[p]
        return buf.at[rows(owner_rep), col : col + width]

    order = [(k + chips // 2) % chips for k in range(chips)]
    order = [k for k in order if k]

    def weight_send(p, k):
        to = (chip + k) % chips
        return remote(
            piece_src(p, to % QUARTERS), piece_dst(p, rep), w_send.at[p, k], w_recv.at[p, chip], dev(to)
        )

    def weight_from(p, k):
        source = (chip + chips - k) % chips
        owner = source * CORES + core
        return remote(
            piece_dst(p, owner), piece_dst(p, owner), w_send.at[p, k], w_recv.at[p, source], dev(source)
        )

    def own_local(p):
        return pltpu.make_async_copy(piece_src(p, quarter), piece_dst(p, rep), l_sem.at[3 + p])

    def own_pass(p):
        return remote(piece_src(p, quarter), piece_dst(p, rep), f_send.at[p, 0], f_recv.at[p, 0], sibling)

    def passed(p, k):
        source = (chip + chips - k) % chips
        owner = source * CORES + core
        return remote(piece_dst(p, owner), piece_dst(p, owner), f_send.at[p, k], f_recv.at[p, k], sibling)

    def passed_in(p, k):
        source = (chip + chips - k) % chips
        owner = source * CORES + (1 - core)
        return remote(piece_dst(p, owner), piece_dst(p, owner), f_send.at[p, k], f_recv.at[p, k], sibling)

    def start_chunk(c):
        for k in order:
            for p in chunks[c]:
                weight_send(p, k).start()
        for p in chunks[c]:
            own_local(p).start()
            own_pass(p).start()

    def pass_chunk(c):
        for k in order:
            for p in chunks[c]:
                weight_from(p, k).wait_recv()
                passed(p, k).start()

    def finish_chunk(c):
        for p in chunks[c]:
            own_local(p).wait()
            for k in range(chips):
                passed_in(p, k).wait_recv()

    for copy in (z_x, z_t, x_own, x_gain, y_own, y_t, *local):
        copy.start()
    start_chunk(0)
    z_x.wait_recv()
    y_two.start()
    x_two.start()
    z_t.wait_recv()
    y_t2.start()
    for c in range(1, len(chunks)):
        start_chunk(c)
    y_own.wait_recv()
    x_three.start()
    y_two.wait_recv()
    x_four.start()
    pass_chunk(0)
    for copy in (y_t, y_t2, x_own, x_gain, x_two, x_three, x_four):
        copy.wait_recv()
    for copy in local:
        copy.wait()
    for copy in (z_x, z_t, x_own, x_gain, y_own, y_t, y_two, y_t2, x_two, x_three, x_four):
        copy.wait_send()

    total = QUARTERS * seqs
    tall = 32

    gain_row = g_buf[...].astype(jnp.float32)[None, :]

    @pl.loop(0, total // tall)
    def _(i):
        at_rows = pl.ds(pl.multiple_of(i * tall, tall), tall)
        values = x_buf[at_rows, :].astype(jnp.float32)
        mean_square = jnp.mean(values * values, axis=1, keepdims=True)
        x_buf[at_rows, :] = (values * lax.rsqrt(mean_square + norm_eps) * gain_row).astype(jnp.bfloat16)

    per_group = QH // KVH + 2
    deep = 2 * seqs

    def compute(c):
        @pl.loop(0, total // deep)
        def _(i):
            at_rows = pl.ds(pl.multiple_of(i * deep, deep), deep)
            chosen = x_buf[at_rows, :]
            if c == 0:
                table = t_buf[at_rows, :]
                swapped = pltpu.roll(table, HD // 2, 1)
                lane = lax.broadcasted_iota(jnp.int32, table.shape, 1)
                low = lane < HD // 2
                cosine = jnp.where(low, table, swapped)
                sine_part = jnp.where(low, -swapped, table)
                for n in range(0, qcols, 2 * HD):
                    wide = jnp.dot(chosen, wq_buf[:, n : n + 2 * HD], preferred_element_type=jnp.float32)
                    for s in range(2):
                        head = wide[:, s * HD : (s + 1) * HD]
                        if (n // HD + s) % per_group < per_group - 1:
                            head = head * cosine + pltpu.roll(head, HD // 2, 1) * sine_part
                        q_res[at_rows, n + s * HD : n + (s + 1) * HD] = head.astype(jnp.bfloat16)
            else:
                width = widths[c - 1]
                both = jnp.dot(chosen, gu_bufs[c - 1][...], preferred_element_type=jnp.float32)
                gate, up = both[:, :width], both[:, width:]
                h_res[c - 1][at_rows, :] = (gate / (1.0 + jnp.exp(-gate)) * up).astype(jnp.bfloat16)

    def result(c, q):
        place = (q % 2) * 2 + q // 2
        if c == 0:
            return q_res.at[rows(place)], lambda mover: q_out.at[:, cols(mover * qcols, qcols)]
        offset = sum(widths[: c - 1])
        return h_res[c - 1].at[rows(place)], lambda mover: h_out.at[:, cols(mover * hcols + offset, widths[c - 1])]

    def out_send(c, k):
        to = (quarter + k) % QUARTERS
        src, dst = result(c, to)
        return remote(src, dst(quarter), o_send.at[c, k], o_recv.at[c, k], dev(half * QUARTERS + to))

    def out_from(c, k):
        source = (quarter + QUARTERS - k) % QUARTERS
        src, dst = result(c, quarter)
        return remote(src, dst(source), o_send.at[c, k], o_recv.at[c, k], dev(half * QUARTERS + source))

    def out_local(c):
        src, dst = result(c, quarter)
        return pltpu.make_async_copy(src, dst(quarter), l_sem.at[3 + len(pieces) + c])

    def ship(c):
        for k in range(1, QUARTERS):
            out_send(c, k).start()
        out_local(c).start()

    for c in range(len(chunks)):
        if c:
            pass_chunk(c)
        finish_chunk(c)
        compute(c)
        ship(c)
        if c + 99 < len(chunks):
            start_chunk(c + 99)

    for c in range(len(chunks)):
        for p in chunks[c]:
            for k in range(1, chips):
                weight_send(p, k).wait_send()
                passed(p, k).wait_send()
            own_pass(p).wait_send()
        out_local(c).wait()
        for k in range(1, QUARTERS):
            out_send(c, k).wait_send()
            out_from(c, k).wait_recv()


def fused(chips, positions, activations, norm_gain, qkv_weight, gate_up_weight):
    seqs, feats = activations.shape
    depth, qkv_cols = qkv_weight.shape
    qcols = qkv_cols // QUARTERS
    hcols = gate_up_weight.shape[1] // 2 // QUARTERS
    widths = widths_of(hcols)
    rank = chips * CORES
    table = jnp.concatenate(angle_parts(positions), axis=1)
    gains = norm_gain
    bf16, f32 = jnp.bfloat16, jnp.float32
    pieces, chunks = 1 + 2 * len(widths), 1 + len(widths)
    dma = pltpu.SemaphoreType.DMA
    scratch = [
        pltpu.VMEM((QUARTERS * seqs, 2 * feats), bf16),
        pltpu.VMEM((QUARTERS * seqs, HD), f32),
        pltpu.VMEM((2 * feats,), bf16),
        pltpu.VMEM((QUARTERS * seqs, qcols), bf16),
        pltpu.VMEM((rank * depth, qcols), bf16),
        *[pltpu.VMEM((rank * depth, 2 * w), bf16) for w in widths],
        *[pltpu.VMEM((QUARTERS * seqs, w), bf16) for w in widths],
        dma((pieces, chips)),
        dma((pieces, chips)),
        dma((pieces, chips)),
        dma((pieces, chips)),
        dma((chunks, QUARTERS)),
        dma((chunks, QUARTERS)),
        dma((11,)),
        dma((11,)),
        dma((3 + pieces + chunks,)),
    ]
    plan = (chips, seqs, feats, qcols, hcols, tuple(widths))
    anywhere = pl.BlockSpec(memory_space=pl.ANY)
    return pl.pallas_call(
        functools.partial(kernel, plan),
        out_shape=(
            pltpu.VMEM((seqs, qkv_cols), bf16),
            pltpu.VMEM((seqs, hcols * QUARTERS), bf16),
        ),
        in_specs=[anywhere] * 5,
        out_specs=(pl.BlockSpec(memory_space=pltpu.VMEM), pl.BlockSpec(memory_space=pltpu.VMEM)),
        scratch_shapes=scratch,
        compiler_params=pltpu.CompilerParams(
            collective_id=0, has_side_effects=True, vmem_limit_bytes=60 * 1024 * 1024
        ),
    )(table, activations, gains, qkv_weight, gate_up_weight)


def per_device(reps, tps, positions, activations, norm_gain, qkv_weight, gate_up_weight):
    chips = reps // CORES
    seqs, depth = activations.shape[0], qkv_weight.shape[0]
    fits = (
        chips == 2 * QUARTERS
        and tps == 2
        and seqs == depth
        and seqs % 32 == 0
        and qkv_weight.shape[1] % (QUARTERS * (QH // KVH + 2) * HD) == 0
        and gate_up_weight.shape[1] % (2 * QUARTERS * HD) == 0
    )
    step = functools.partial(fused, chips) if fits else plain
    return step(positions, activations, norm_gain, qkv_weight, gate_up_weight)


def solution(mesh):
    placed = (P("rep"), P("rep", "tp"), P("tp"), P("rep", "tp"), P("rep", "tp"))
    return jax.shard_map(
        functools.partial(per_device, mesh.shape["rep"], mesh.shape["tp"]),
        mesh=mesh,
        in_specs=placed,
        out_specs=(P("rep", "tp"), P("rep", "tp")),
        check_vma=False,
    )
```
